32 devices in a mesh: dp: 32 (over z, y, x, core).
Axes of the slice: x: 2, y: 2, z: 4, core: 2. Of those that a mesh axis runs over, the one named last changes fastest.
Arguments:
- grads: float32 [32, 163840], P('dp'), may hold values from -6 to 6
- master: float32 [163840], P('dp')
- moment1: float32 [163840], P('dp'), may hold values from -4 to 4
- moment2: float32 [163840], P('dp'), may hold values from 0.1 to 2
- tensor_rows: int32 [8], replicated, may hold values from 1 to 16, 32 in all
- step_count: int32 [1], replicated, may hold values from 1 to 19
Outputs:
- new_weights: bfloat16 [163840], replicated
- new_master: float32 [163840], P('dp')
- new_moment1: float32 [163840], P('dp')
- new_moment2: float32 [163840], P('dp')
The draws below stay inside these ranges and needn't reach their ends.
All inputs are finite; a program needn't handle non-finite values.
Results may differ from the reference program's by a relative error of at most 0.001.
Values may be sent and summed in bfloat16 or wider, within the bound.
A program may use at most 64 MiB of HBM per device.

```python
import math
import jax
import jax.numpy as jnp
import numpy as np
from jax import lax

D = 5120
NSEG = 8
ROWS = 32
P_SIZE = 163840
N_DP = 32


def draw_master(key, part):
    base_key, row_key, col_key = jax.random.split(jax.random.fold_in(key, 17), 3)
    base = jax.random.normal(base_key, (ROWS, D), jnp.float32)
    position = jnp.arange(ROWS, dtype=jnp.float32) / jnp.float32(ROWS)
    row_scale = jnp.exp(jax.random.uniform(row_key, (ROWS, 1), jnp.float32, 0.0, math.log(10.0)))
    row_scale = row_scale * jnp.power(3.0, position)[:, None]
    col_scale = jnp.exp(jax.random.uniform(col_key, (1, D), jnp.float32, 0.0, math.log(4.0)))
    return (0.1 * base * row_scale * col_scale).reshape(P_SIZE).astype(jnp.float32)


def strengthened(entries, rng, source, target, shards_of, factor):
    def block_of(dim):
        return (jnp.arange(entries.shape[dim]) // (entries.shape[dim] // shards_of)).reshape((-1,) + (1,) * (entries.ndim - 1 - dim))

    first = jax.random.permutation(rng, shards_of)[block_of(target)]
    far = (block_of(target) + shards_of // 2) % shards_of
    return jnp.where((block_of(source) == first) | (block_of(source) == far), factor * entries, entries)


def shard_levels(own_key, extent, pieces, least, largest):
    def one(dim, parts):
        heights = jax.random.uniform(jax.random.fold_in(jax.random.fold_in(own_key, 6), dim), (parts,), jnp.float32, least / len(pieces), largest / len(pieces))
        return jnp.repeat(jnp.exp(heights), extent[dim] // parts).reshape((-1,) + (1,) * (len(extent) - dim - 1))

    factor_of = one(*pieces[0])
    for cut in pieces[1:]:
        factor_of = factor_of * one(*cut)
    return factor_of


def split_up(number_of, total, bound, lean):
    weights = [(1 << 20) // math.isqrt(rank ** lean) + 1 for rank in range(2, number_of + 1)]
    surplus, given = total - bound - (number_of - 1), [1] * (number_of - 1)
    while surplus > 0:
        candidates = [i for i in range(number_of - 1) if given[i] < bound]
        pool, remaining = sum([weights[i] for i in candidates]), surplus
        for i in candidates:
            addition = min(bound - given[i], max(1, remaining * weights[i] // pool), surplus)
            given[i] = given[i] + addition
            surplus = surplus - addition
    return np.array([bound] + given)


def uneven_parts(rng, count, total, most, skew):
    if count == 2:
        one = jax.random.randint(rng, (), max(1, total - most), min(most, total - 1) + 1)
        return jnp.stack([one, total - one])
    sizes = jnp.asarray(split_up(count, total, most, skew), jnp.int32)
    pairs = (count - 1) // 2
    giver, taker = sizes[1:1 + 2 * pairs:2], sizes[2:2 + 2 * pairs:2]
    margin = jnp.minimum(giver - 1, most - taker)
    passed = jax.random.randint(jax.random.fold_in(rng, 1), (pairs,), 0, 1 << 20) % (margin + 1)
    sizes = sizes.at[1:1 + 2 * pairs:2].set(giver - passed).at[2:2 + 2 * pairs:2].set(taker + passed)
    return sizes[jax.random.permutation(jax.random.fold_in(rng, 2), count)]


def noise(own_key, extent, spread, reach, cuts=(), held_as=jnp.bfloat16):
    loudness = shard_levels(own_key, extent, cuts, -0.22, 0.18) if cuts else 1.0
    entries = jax.random.normal(own_key, extent, jnp.float32) * spread * loudness
    return jnp.minimum(jnp.maximum(entries, -reach), reach).astype(held_as)


def heavy_noise(key, shape, deviation, limit, cuts, heavy, kind=jnp.bfloat16):
    result = deviation * jax.random.normal(key, shape, jnp.float32)
    if cuts:
        result = result * shard_levels(key, shape, cuts, -0.22, 0.18)
    return jnp.clip(strengthened(result, jax.random.fold_in(key, 3), *heavy), -limit, limit).astype(kind)


def setup_inputs(seed: int = 0) -> dict:
    streams_of = jax.random.split(jax.random.key(seed), 7)
    grads = heavy_noise(streams_of[0], (N_DP, P_SIZE), 1.0, 6.0, ((0, 32),), (0, 1, 32, 2.75), jnp.float32)
    master = draw_master(jax.random.fold_in(streams_of[6], 71), 0)
    moment1 = noise(streams_of[2], (P_SIZE,), 0.5, 4.0, ((0, 32),), jnp.float32)
    moment2 = jnp.clip(jnp.exp(math.log(2.0) - 2.9957323 * jax.random.uniform(streams_of[3], (P_SIZE,), jnp.float32) ** shard_levels(streams_of[3], (P_SIZE,), ((0, 32),), -0.2, 0.2)), 0.1, 2.0)
    tensor_rows = uneven_parts(streams_of[4], NSEG, ROWS, ROWS // 2, 2).astype(jnp.int32)
    step_count = jax.random.randint(streams_of[5], (1,), 1, 20).astype(jnp.int32)
    return dict(grads=grads, master=master, moment1=moment1, moment2=moment2, tensor_rows=tensor_rows, step_count=step_count)


def reference(grads, master, moment1, moment2, tensor_rows, step_count):
    grad = lax.optimization_barrier(jnp.sum(grads, axis=0)) / jnp.float32(N_DP)
    new_moment1 = 0.9 * moment1 + 0.1 * grad
    new_moment2 = 0.999 * moment2 + 0.001 * grad * grad
    steps = step_count[0].astype(jnp.float32)
    first = new_moment1 / (1.0 - jnp.power(jnp.float32(0.9), steps))
    second = new_moment2 / (1.0 - jnp.power(jnp.float32(0.999), steps))
    update = first / (jnp.sqrt(second) + 1e-06) + 0.1 * master
    ends = jnp.cumsum(tensor_rows).astype(jnp.int32)
    starts = ends - tensor_rows
    row_index = jnp.arange(ROWS, dtype=jnp.int32)
    onehot = ((row_index[:, None] >= starts[None, :]) & (row_index[:, None] < ends[None, :])).astype(jnp.float32)
    weight_rows = master.reshape(ROWS, D)
    update_rows = update.reshape(ROWS, D)
    row_wsq = lax.optimization_barrier(jnp.sum(weight_rows * weight_rows, axis=1))
    row_usq = lax.optimization_barrier(jnp.sum(update_rows * update_rows, axis=1))
    wsq = lax.optimization_barrier(jnp.sum(onehot * row_wsq[:, None], axis=0))
    usq = lax.optimization_barrier(jnp.sum(onehot * row_usq[:, None], axis=0))
    ratio = jnp.sqrt(wsq / (usq + 1e-06))
    row_ratio = lax.optimization_barrier(jnp.sum(onehot * ratio[None, :], axis=1))
    new_master = (weight_rows - 0.2 * row_ratio[:, None] * update_rows).reshape(P_SIZE)
    new_weights = new_master.astype(jnp.bfloat16)
    return (new_weights, new_master, new_moment1, new_moment2)
```

```python
import functools

import jax
import jax.numpy as jnp
import numpy as np
from jax import lax
from jax.experimental import pallas as pl
from jax.experimental.pallas import tpu as pltpu
from jax.sharding import PartitionSpec as P

LANES = 128
BETA1, BETA2 = 0.9, 0.999
STEP_BITS = 8


def levels(count):
    chips = count // 2
    bits = chips.bit_length() - 1
    plane = 1 << ((bits + 1) // 2)
    return chips // plane, plane


def flipped(value, mask):
    bit = 1
    while bit <= mask:
        if mask & bit:
            value = value + bit * (1 - 2 * (value // bit % 2))
        bit *= 2
    return value


def power(base, step):
    result = jnp.ones(step.shape, jnp.float32)
    for bit in range(STEP_BITS):
        factor = float(np.float32(float(np.float32(base)) ** (2**bit)))
        result = result * jnp.where((step // 2**bit) % 2 == 1, factor, 1.0)
    return result


def kernel(
    count, line, plane, width,
    grads, master, moment1, moment2, rows_ref, step_ref,
    weights_out, master_out, moment1_out, moment2_out,
    theirs, ours, pair_send, pair_recv, own, plane_send, plane_recv,
    total, line_send, line_recv, masters, updates, m1, m2, m1_new, m2_new,
    master_new, weights, wsums, usums, ratios,
    local_sem, send_sem, recv_sem,
):
    me = lax.axis_index("dp")
    core = me % 2
    xy = me // 2 % plane
    z = me // (2 * plane)
    other = 1 - core
    order = list(range(plane - 1, -1, -1))
    far_first = list(range(line - 1, 0, -1))
    partner = me + 1 - 2 * core

    def plane_peer(mask):
        return (z * plane + flipped(xy, mask)) * 2 + core

    def line_peer(mask):
        return (flipped(z, mask) * plane + xy) * 2 + core

    peers = [partner] + [plane_peer(k) for k in range(1, plane)]
    peers += [line_peer(k) for k in range(1, line)]
    barrier = pltpu.get_barrier_semaphore()
    for peer in peers:
        pl.semaphore_signal(barrier, inc=1, device_id=(peer,), device_id_type=pl.DeviceIdType.MESH)

    used = {"local": 0, "remote": 0}
    sent = []

    def local(source, target):
        copy = pltpu.make_async_copy(source, target, local_sem.at[used["local"]])
        used["local"] += 1
        copy.start()
        return copy

    def remote(source, target, peer):
        slot = used["remote"]
        used["remote"] += 1
        copy = pltpu.make_async_remote_copy(
            src_ref=source, dst_ref=target,
            send_sem=send_sem.at[slot], recv_sem=recv_sem.at[slot],
            device_id=(peer,), device_id_type=pl.DeviceIdType.MESH,
        )
        copy.start()
        sent.append(copy)
        return copy

    their_loads = [local(grads.at[:, flipped(xy, k), other], theirs.at[k]) for k in order]
    master_load = local(master, masters.at[core, xy, z])
    our_loads = [local(grads.at[:, flipped(xy, k), core], ours.at[k]) for k in order]
    m1_load = local(moment1, m1)
    m2_load = local(moment2, m2)

    for k, load in zip(order, their_loads):
        load.wait()
        pair_send[k] = theirs[k].reshape(line * width, LANES).astype(jnp.bfloat16)
    master_load.wait()
    pl.semaphore_wait(barrier, len(peers))

    pair_copies = [remote(pair_send.at[k], pair_recv.at[k], partner) for k in order]
    row = masters.at[core, xy, z]
    master_line = [remote(row, row, line_peer(k)) for k in far_first]

    plane_copies = []
    for k, load, copy in zip(order, our_loads, pair_copies):
        load.wait()
        copy.wait_recv()
        chip = ours[k].reshape(line * width, LANES) + pair_recv[k].astype(jnp.float32)
        if k:
            plane_send[k - 1] = chip.astype(jnp.bfloat16)
            plane_copies.append((k, remote(plane_send.at[k - 1], plane_recv.at[k - 1], plane_peer(k))))
        else:
            own[...] = chip

    for copy in master_line:
        copy.wait_recv()
    column = masters.at[core, xy]
    master_plane = [(k, remote(column, column, plane_peer(k))) for k in order if k]
    master_pair = [remote(column, column, partner)]

    acc = own[...]
    for k, copy in plane_copies:
        copy.wait_recv()
        acc = acc + plane_recv[k - 1].astype(jnp.float32)
    total[...] = acc.reshape(line, width, LANES)
    line_copies = []
    for k in far_first:
        line_send[k - 1] = total[flipped(z, k)].astype(jnp.bfloat16)
        line_copies.append((k, remote(line_send.at[k - 1], line_recv.at[k - 1], line_peer(k))))

    m1_load.wait()
    m2_load.wait()
    step = jnp.full((8, LANES), step_ref[0], jnp.int32)
    first_scale = (1.0 - power(BETA1, step))[:1]
    second_scale = (1.0 - power(BETA2, step))[:1]
    grad = total[z]
    for k, copy in line_copies:
        copy.wait_recv()
        grad = grad + line_recv[k - 1].astype(jnp.float32)
    grad = grad / jnp.float32(count)
    new_m1 = 0.9 * m1[...] + 0.1 * grad
    new_m2 = 0.999 * m2[...] + 0.001 * grad * grad
    update = (new_m1 / first_scale) / (jnp.sqrt(new_m2 / second_scale) + 1e-06)
    updates[core, xy, z] = update + 0.1 * masters[core, xy, z]
    row = updates.at[core, xy, z]
    update_line = [remote(row, row, line_peer(k)) for k in far_first]
    m1_new[...] = new_m1
    m2_new[...] = new_m2
    stores = [local(m1_new, moment1_out), local(m2_new, moment2_out)]

    def square_sums(table, sums, side, at):
        start = (side * plane + at) * line
        for j in range(line):
            values = table[side, at, j].reshape(width // 8, 8, LANES)
            sums[start + j] = jnp.sum(values * values, axis=0)

    square_sums(masters, wsums, core, xy)
    for k, copy in master_plane:
        copy.wait_recv()
        at = flipped(xy, k)
        chunk = masters.at[core, at]
        master_pair.append(remote(chunk, chunk, partner))
        square_sums(masters, wsums, core, at)

    for copy in update_line:
        copy.wait_recv()
    column = updates.at[core, xy]
    update_plane = [(k, remote(column, column, plane_peer(k))) for k in order if k]
    update_pair = [remote(column, column, partner)]
    square_sums(updates, usums, core, xy)

    pair_masks = [0] + [k for k in order if k]
    for k, copy in zip(pair_masks, master_pair):
        copy.wait_recv()
        square_sums(masters, wsums, other, flipped(xy, k))

    index0 = lax.broadcasted_iota(jnp.int32, (count, count), 0)
    index1 = lax.broadcasted_iota(jnp.int32, (count, count), 1)

    def tensor_of(index):
        natural = (index % line * plane + index // line % plane) * 2 + index // (line * plane)
        end = jnp.int32(0)
        tensor = jnp.zeros(index.shape, jnp.int32)
        for k in range(rows_ref.shape[0]):
            end = end + rows_ref[k]
            tensor = tensor + (natural >= end).astype(jnp.int32)
        return tensor

    same = tensor_of(index0) == tensor_of(index1)

    def over_tensor(sums):
        per_row = jnp.sum(jnp.sum(sums[...], axis=1), axis=1, keepdims=True)
        return jnp.sum(jnp.where(same, per_row, 0.0), axis=0, keepdims=True)

    wsq = over_tensor(wsums)

    for k, copy in update_plane:
        copy.wait_recv()
        at = flipped(xy, k)
        chunk = updates.at[core, at]
        update_pair.append(remote(chunk, chunk, partner))
        square_sums(updates, usums, core, at)
    for k, copy in zip(pair_masks, update_pair):
        copy.wait_recv()
        square_sums(updates, usums, other, flipped(xy, k))

    ratio = jnp.sqrt(wsq / (over_tensor(usums) + 1e-06))
    column = jnp.sum(jnp.where(index0 == index1, ratio, 0.0), axis=1, keepdims=True)
    ratios[...] = jnp.broadcast_to(0.2 * column, (count, LANES))

    def new_row(side, at, j):
        scale = ratios[pl.ds((side * plane + at) * line + j, 1), :]
        return masters[side, at, j] - scale * updates[side, at, j]

    master_new[...] = new_row(core, xy, z)
    stores.append(local(master_new, master_out))

    base = used["local"]

    @pl.loop(0, line)
    def _(j):
        for at in range(plane):
            both = jnp.concatenate([new_row(0, at, j), new_row(1, at, j)], axis=0)
            weights[j, at] = both.astype(jnp.bfloat16)
        pltpu.make_async_copy(weights.at[j], weights_out.at[j], local_sem.at[base + j]).start()

    for j in range(line):
        stores.append(pltpu.make_async_copy(weights.at[j], weights_out.at[j], local_sem.at[base + j]))
    for copy in stores:
        copy.wait()
    for copy in sent:
        copy.wait_send()


def body(grads, master, moment1, moment2, tensor_rows, step_count):
    count = lax.axis_size("dp")
    line, plane = levels(count)
    width = master.shape[0] // LANES
    row = (width, LANES)
    f32, bf16 = jnp.float32, jnp.bfloat16
    anywhere = pl.BlockSpec(memory_space=pl.ANY)
    scalars = pl.BlockSpec(memory_space=pltpu.SMEM)
    tall = (line * width, LANES)
    remotes = plane + 3 * (line - 1 + plane - 1) + 2 * plane
    outs = pl.pallas_call(
        functools.partial(kernel, count, line, plane, width),
        out_shape=(
            jax.ShapeDtypeStruct((line, plane, 2 * width, LANES), bf16),
            jax.ShapeDtypeStruct(row, f32),
            jax.ShapeDtypeStruct(row, f32),
            jax.ShapeDtypeStruct(row, f32),
        ),
        in_specs=[anywhere] * 4 + [scalars] * 2,
        out_specs=(anywhere,) * 4,
        scratch_shapes=[
            pltpu.VMEM((plane, line) + row, f32),
            pltpu.VMEM((plane, line) + row, f32),
            pltpu.VMEM((plane,) + tall, bf16),
            pltpu.VMEM((plane,) + tall, bf16),
            pltpu.VMEM(tall, f32),
            pltpu.VMEM((plane - 1,) + tall, bf16),
            pltpu.VMEM((plane - 1,) + tall, bf16),
            pltpu.VMEM((line,) + row, f32),
            pltpu.VMEM((line - 1,) + row, bf16),
            pltpu.VMEM((line - 1,) + row, bf16),
            pltpu.VMEM((2, plane, line) + row, f32),
            pltpu.VMEM((2, plane, line) + row, f32),
            pltpu.VMEM(row, f32),
            pltpu.VMEM(row, f32),
            pltpu.VMEM(row, f32),
            pltpu.VMEM(row, f32),
            pltpu.VMEM(row, f32),
            pltpu.VMEM((line, plane, 2 * width, LANES), bf16),
            pltpu.VMEM((count, 8, LANES), f32),
            pltpu.VMEM((count, 8, LANES), f32),
            pltpu.VMEM((count, LANES), f32),
            pltpu.SemaphoreType.DMA((2 * plane + 6 + line,)),
            pltpu.SemaphoreType.DMA((remotes,)),
            pltpu.SemaphoreType.DMA((remotes,)),
        ],
        compiler_params=pltpu.CompilerParams(
            collective_id=0, has_side_effects=True, vmem_limit_bytes=48 * 1024 * 1024
        ),
        name="lamb",
    )(
        grads.reshape(line, plane, 2, width, LANES),
        master.reshape(row), moment1.reshape(row), moment2.reshape(row),
        tensor_rows, step_count,
    )
    return tuple(out.reshape(-1) for out in outs)


def solution(mesh):
    placed = (P("dp", None), P("dp"), P("dp"), P("dp"), P(), P())
    return jax.shard_map(
        body,
        mesh=mesh,
        in_specs=placed,
        out_specs=(P(), P("dp"), P("dp"), P("dp")),
        check_vma=False,
    )
```

```python
import functools

import jax
import jax.numpy as jnp
import numpy as np
from jax import lax
from jax.experimental import pallas as pl
from jax.experimental.pallas import tpu as pltpu
from jax.sharding import PartitionSpec as P

LANES = 128
BETA1, BETA2 = 0.9, 0.999
STEP_BITS = 8


def levels(count):
    chips = count // 2
    bits = chips.bit_length() - 1
    plane = 1 << ((bits + 1) // 2)
    return chips // plane, plane


def flipped(value, mask):
    bit = 1
    while bit <= mask:
        if mask & bit:
            value = value + bit * (1 - 2 * (value // bit % 2))
        bit *= 2
    return value


def power(base, step):
    result = jnp.ones(step.shape, jnp.float32)
    for bit in range(STEP_BITS):
        factor = float(np.float32(float(np.float32(base)) ** (2**bit)))
        result = result * jnp.where((step // 2**bit) % 2 == 1, factor, 1.0)
    return result


def kernel(
    count, line, plane,
    grads, master, moment1, moment2, rows_in, step_ref,
    masters, updates, ratios, m1_new, m2_new,
    theirs, ours, pair_send, pair_recv, plane_send, plane_recv,
    line_send, line_recv, m1, m2, wsums, usums, rows_ref,
    local_sem, send_sem, recv_sem,
):
    me = lax.axis_index("dp")
    core = me % 2
    xy = me // 2 % plane
    z = me // (2 * plane)
    other = 1 - core
    partner = me + 1 - 2 * core
    far_first = list(range(line - 1, 0, -1))
    diagonal_first = list(range(plane - 1, 0, -1))

    def plane_peer(mask):
        return (z * plane + flipped(xy, mask)) * 2 + core

    def line_peer(mask):
        return (flipped(z, mask) * plane + xy) * 2 + core

    peers = [partner] + [plane_peer(k) for k in range(1, plane)]
    peers += [line_peer(k) for k in range(1, line)]
    barrier = pltpu.get_barrier_semaphore()
    for peer in peers:
        pl.semaphore_signal(barrier, inc=1, device_id=(peer,), device_id_type=pl.DeviceIdType.MESH)

    used = {"local": 0, "remote": 0}
    sent = []

    def local(source, target):
        copy = pltpu.make_async_copy(source, target, local_sem.at[used["local"]])
        used["local"] += 1
        copy.start()
        return copy

    def remote(source, target, peer):
        slot = used["remote"]
        used["remote"] += 1
        copy = pltpu.make_async_remote_copy(
            src_ref=source, dst_ref=target,
            send_sem=send_sem.at[slot], recv_sem=recv_sem.at[slot],
            device_id=(peer,), device_id_type=pl.DeviceIdType.MESH,
        )
        copy.start()
        sent.append(copy)
        return copy

    def share(ref, peer):
        return remote(ref, ref, peer)

    layers = far_first + [0]
    their_loads = [local(grads.at[flipped(z, k), :, other], theirs.at[k]) for k in layers]
    master_load = local(master, masters.at[core, xy, z])
    our_loads = [local(grads.at[flipped(z, k), :, core], ours.at[k]) for k in layers]
    small_loads = [
        local(moment1, m1), local(moment2, m2), local(rows_in, rows_ref)
    ]

    for k, load in zip(layers, their_loads):
        load.wait()
        pair_send[k] = theirs[k].astype(jnp.bfloat16)
    master_load.wait()
    pl.semaphore_wait(barrier, len(peers))

    pair_copies = [remote(pair_send.at[k], pair_recv.at[k], partner) for k in layers]
    master_line = [share(masters.at[core, xy, z], line_peer(k)) for k in far_first]

    plane_copies = {}
    for k, load, copy in zip(layers, our_loads, pair_copies):
        load.wait()
        copy.wait_recv()
        for p in diagonal_first:
            at = flipped(xy, p)
            chip = ours[k, at] + pair_recv[k, at].astype(jnp.float32)
            plane_send[k, p - 1] = chip.astype(jnp.bfloat16)
            plane_copies[k, p] = remote(plane_send.at[k, p - 1], plane_recv.at[k, p - 1], plane_peer(p))

    def plane_sum(k):
        total = ours[k, xy] + pair_recv[k, xy].astype(jnp.float32)
        for p in diagonal_first:
            plane_copies[k, p].wait_recv()
            total = total + plane_recv[k, p - 1].astype(jnp.float32)
        return total

    line_copies = []
    for k in far_first:
        line_send[k - 1] = plane_sum(k).astype(jnp.bfloat16)
        line_copies.append((k, remote(line_send.at[k - 1], line_recv.at[k - 1], line_peer(k))))

    grad = plane_sum(0)
    for copy in small_loads:
        copy.wait()
    step = jnp.full((8, LANES), step_ref[0], jnp.int32)
    first_scale = 1.0 - power(BETA1, step)
    second_scale = 1.0 - power(BETA2, step)

    for copy in master_line:
        copy.wait_recv()
    column = masters.at[core, xy]
    master_plane = [(p, share(column, plane_peer(p))) for p in diagonal_first]
    master_pair = [share(column, partner)]

    for k, copy in line_copies:
        copy.wait_recv()
        grad = grad + line_recv[k - 1].astype(jnp.float32)
    grad = grad / jnp.float32(count)
    new_m1 = 0.9 * m1[...] + 0.1 * grad
    new_m2 = 0.999 * m2[...] + 0.001 * grad * grad
    update = (new_m1 / first_scale) / (jnp.sqrt(new_m2 / second_scale) + 1e-06)
    updates[core, xy, z] = update + 0.1 * masters[core, xy, z]
    m1_new[...] = new_m1
    m2_new[...] = new_m2

    update_line = [(k, share(updates.at[core, xy, z], line_peer(k))) for k in far_first]
    update_plane, update_pair = [], []

    def spread(at_z):
        row = updates.at[core, xy, at_z]
        for p in diagonal_first:
            update_plane.append((p, at_z, share(row, plane_peer(p))))
        update_pair.append((xy, at_z, share(row, partner)))

    def square_sum(table, sums, side, at, j):
        values = table[side, at, j]
        sums[(side * plane + at) * line + j] = jnp.sum(values * values, axis=0)

    def square_sums(table, sums, side, at):
        for j in range(line):
            square_sum(table, sums, side, at, j)

    spread(z)
    square_sums(masters, wsums, core, xy)
    for p, copy in master_plane:
        copy.wait_recv()
        at = flipped(xy, p)
        master_pair.append(share(masters.at[core, at], partner))
        square_sums(masters, wsums, core, at)
    for k, copy in reversed(update_line):
        copy.wait_recv()
        spread(flipped(z, k))
    square_sums(updates, usums, core, xy)
    for p, at_z, copy in update_plane:
        copy.wait_recv()
        at = flipped(xy, p)
        update_pair.append((at, at_z, share(updates.at[core, at, at_z], partner)))
        square_sum(updates, usums, core, at, at_z)

    for p, copy in zip([0] + diagonal_first, master_pair):
        copy.wait_recv()
        square_sums(masters, wsums, other, flipped(xy, p))

    index0 = lax.broadcasted_iota(jnp.int32, (count, count), 0)
    index1 = lax.broadcasted_iota(jnp.int32, (count, count), 1)

    def tensor_of(index):
        natural = (index % line * plane + index // line % plane) * 2 + index // (line * plane)
        end = jnp.int32(0)
        tensor = jnp.zeros(index.shape, jnp.int32)
        for k in range(rows_ref.shape[0]):
            end = end + rows_ref[k]
            tensor = tensor + (natural >= end).astype(jnp.int32)
        return tensor

    same = tensor_of(index0) == tensor_of(index1)

    def over_tensor(sums):
        per_row = jnp.sum(jnp.sum(sums[...], axis=1), axis=1, keepdims=True)
        return jnp.sum(jnp.where(same, per_row, 0.0), axis=0, keepdims=True)

    wsq = over_tensor(wsums)

    for at, at_z, copy in update_pair:
        copy.wait_recv()
        square_sum(updates, usums, other, at, at_z)

    ratio = jnp.sqrt(wsq / (over_tensor(usums) + 1e-06))
    column = jnp.sum(jnp.where(index0 == index1, ratio, 0.0), axis=1, keepdims=True)
    ratios[...] = jnp.broadcast_to(0.2 * column, (count, LANES))
    for copy in sent:
        copy.wait_send()


def finish(
    line, plane,
    masters, updates, ratios, m1_new, m2_new,
    weights_out, master_out, moment1_out, moment2_out,
    weights, master_new, sem,
):
    me = lax.axis_index("dp")
    copies = [
        pltpu.make_async_copy(m1_new, moment1_out, sem.at[0]),
        pltpu.make_async_copy(m2_new, moment2_out, sem.at[1]),
    ]
    for copy in copies:
        copy.start()

    def new_row(side, at, j):
        scale = ratios[pl.ds((side * plane + at) * line + j, 1), :]
        return masters[side, at, j] - scale * updates[side, at, j]

    master_new[...] = new_row(me % 2, me // 2 % plane, me // (2 * plane))
    copies.append(pltpu.make_async_copy(master_new, master_out, sem.at[2]))
    copies[-1].start()

    @pl.loop(0, line)
    def _(j):
        for at in range(plane):
            for side in range(2):
                weights[j, at, side] = new_row(side, at, j).astype(jnp.bfloat16)
        pltpu.make_async_copy(weights.at[j], weights_out.at[j], sem.at[3 + j]).start()

    for j in range(line):
        copies.append(pltpu.make_async_copy(weights.at[j], weights_out.at[j], sem.at[3 + j]))
    for copy in copies:
        copy.wait()


def pinned(array):
    return pltpu.with_memory_space_constraint(array, pltpu.HBM)


def body(grads, master, moment1, moment2, tensor_rows, step_count):
    count = lax.axis_size("dp")
    line, plane = levels(count)
    row = (master.shape[0] // (8 * LANES), 8, LANES)
    f32, bf16 = jnp.float32, jnp.bfloat16
    hbm = pl.BlockSpec(memory_space=pltpu.HBM)
    vmem = pl.BlockSpec(memory_space=pltpu.VMEM)
    table = (2, plane, line) + row
    remotes = line + line * (plane - 1) + 2 * (line - 1) + plane - 1 + plane
    remotes += line - 1 + line * (plane - 1) + line * plane
    state = pl.pallas_call(
        functools.partial(kernel, count, line, plane),
        out_shape=(
            jax.ShapeDtypeStruct(table, f32),
            jax.ShapeDtypeStruct(table, f32),
            jax.ShapeDtypeStruct((count, LANES), f32),
            jax.ShapeDtypeStruct(row, f32),
            jax.ShapeDtypeStruct(row, f32),
        ),
        in_specs=[hbm] * 5 + [pl.BlockSpec(memory_space=pltpu.SMEM)],
        out_specs=(vmem,) * 5,
        scratch_shapes=[
            pltpu.VMEM((line, plane) + row, f32),
            pltpu.VMEM((line, plane) + row, f32),
            pltpu.VMEM((line, plane) + row, bf16),
            pltpu.VMEM((line, plane) + row, bf16),
            pltpu.VMEM((line, plane - 1) + row, bf16),
            pltpu.VMEM((line, plane - 1) + row, bf16),
            pltpu.VMEM((line - 1,) + row, bf16),
            pltpu.VMEM((line - 1,) + row, bf16),
            pltpu.VMEM(row, f32),
            pltpu.VMEM(row, f32),
            pltpu.VMEM((count, 8, LANES), f32),
            pltpu.VMEM((count, 8, LANES), f32),
            pltpu.SMEM(tensor_rows.shape, jnp.int32),
            pltpu.SemaphoreType.DMA((2 * line + 4,)),
            pltpu.SemaphoreType.DMA((remotes,)),
            pltpu.SemaphoreType.DMA((remotes,)),
        ],
        compiler_params=pltpu.CompilerParams(
            collective_id=0, has_side_effects=True, vmem_limit_bytes=40 * 1024 * 1024
        ),
        name="exchange",
    )(
        pinned(grads.reshape((line, plane, 2) + row)),
        pinned(master.reshape(row)), pinned(moment1.reshape(row)), pinned(moment2.reshape(row)),
        pinned(tensor_rows), step_count,
    )
    outs = pl.pallas_call(
        functools.partial(finish, line, plane),
        out_shape=(
            jax.ShapeDtypeStruct((line, plane, 2) + row, bf16),
            jax.ShapeDtypeStruct(row, f32),
            jax.ShapeDtypeStruct(row, f32),
            jax.ShapeDtypeStruct(row, f32),
        ),
        in_specs=[vmem] * 5,
        out_specs=(hbm,) * 4,
        scratch_shapes=[
            pltpu.VMEM((line, plane, 2) + row, bf16),
            pltpu.VMEM(row, f32),
            pltpu.SemaphoreType.DMA((3 + line,)),
        ],
        compiler_params=pltpu.CompilerParams(vmem_limit_bytes=24 * 1024 * 1024),
        name="finish",
    )(*state)
    return tuple(out.reshape(-1) for out in outs)


def solution(mesh):
    placed = (P("dp", None), P("dp"), P("dp"), P("dp"), P(), P())
    return jax.shard_map(
        body,
        mesh=mesh,
        in_specs=placed,
        out_specs=(P(), P("dp"), P("dp"), P("dp")),
        check_vma=False,
    )
```

```python
import functools

import jax
import jax.numpy as jnp
import numpy as np
from jax import lax
from jax.experimental import pallas as pl
from jax.experimental.pallas import tpu as pltpu
from jax.sharding import PartitionSpec as P

LANES = 128
BETA1, BETA2 = 0.9, 0.999
STEP_BITS = 8


def levels(count):
    chips = count // 2
    bits = chips.bit_length() - 1
    plane = 1 << ((bits + 1) // 2)
    return chips // plane, plane


def flipped(value, mask):
    bit = 1
    while bit <= mask:
        if mask & bit:
            value = value + bit * (1 - 2 * (value // bit % 2))
        bit *= 2
    return value


def power(base, step):
    result = jnp.ones(step.shape, jnp.float32)
    for bit in range(STEP_BITS):
        factor = float(np.float32(float(np.float32(base)) ** (2**bit)))
        result = result * jnp.where((step // 2**bit) % 2 == 1, factor, 1.0)
    return result


def kernel(
    count, line, plane,
    grads, master, moment1, moment2, rows_in, step_ref,
    masters, guesses, deltas, ratios, m1_new, m2_new, mine,
    theirs, ours, pair_send, pair_recv, plane_send, plane_recv,
    line_send, line_recv, m1, m2, wsums, usums, rows_ref,
    local_sem, send_sem, recv_sem,
):
    me = lax.axis_index("dp")
    core = me % 2
    xy = me // 2 % plane
    z = me // (2 * plane)
    other = 1 - core
    partner = me + 1 - 2 * core
    far_first = list(range(line - 1, 0, -1))
    diagonal_first = list(range(plane - 1, 0, -1))

    def plane_peer(mask):
        return (z * plane + flipped(xy, mask)) * 2 + core

    def line_peer(mask):
        return (flipped(z, mask) * plane + xy) * 2 + core

    peers = [partner] + [plane_peer(k) for k in range(1, plane)]
    peers += [line_peer(k) for k in range(1, line)]
    barrier = pltpu.get_barrier_semaphore()
    for peer in peers:
        pl.semaphore_signal(barrier, inc=1, device_id=(peer,), device_id_type=pl.DeviceIdType.MESH)

    used = {"local": 0, "remote": 0}
    sent = []

    def local(source, target):
        copy = pltpu.make_async_copy(source, target, local_sem.at[used["local"]])
        used["local"] += 1
        copy.start()
        return copy

    def remote(source, target, peer):
        slot = used["remote"]
        used["remote"] += 1
        copy = pltpu.make_async_remote_copy(
            src_ref=source, dst_ref=target,
            send_sem=send_sem.at[slot], recv_sem=recv_sem.at[slot],
            device_id=(peer,), device_id_type=pl.DeviceIdType.MESH,
        )
        copy.start()
        sent.append(copy)
        return copy

    def share(ref, peer):
        return remote(ref, ref, peer)

    layers = far_first + [0]
    their_loads = [local(grads.at[flipped(z, k), :, other], theirs.at[k]) for k in layers]
    master_load = local(master, masters.at[core, xy, z])
    our_loads = [local(grads.at[flipped(z, k), :, core], ours.at[k]) for k in layers]
    moment_loads = [local(moment1, m1), local(moment2, m2)]
    rows_load = local(rows_in, rows_ref)
    step = jnp.full((8, LANES), step_ref[0], jnp.int32)
    first_scale = 1.0 - power(BETA1, step)
    second_scale = 1.0 - power(BETA2, step)

    def update_of(first, second, weight):
        return (first / first_scale) / (jnp.sqrt(second / second_scale) + 1e-06) + 0.1 * weight


    for k, load in zip(layers, their_loads):
        load.wait()
        pair_send[k] = theirs[k].astype(jnp.bfloat16)
    master_load.wait()
    pl.semaphore_wait(barrier, len(peers))

    pair_copies = [remote(pair_send.at[k], pair_recv.at[k], partner) for k in layers]
    early = (masters, guesses)
    early_line = {k: [share(masters.at[core, xy, z], line_peer(k))] for k in far_first}
    for copy in moment_loads:
        copy.wait()
    guess = update_of(0.9 * m1[...], 0.999 * m2[...], masters[core, xy, z]).astype(jnp.bfloat16)
    guesses[core, xy, z] = guess
    early_plane = {p: [] for p in diagonal_first}

    def early_spread(at_z):
        for p in diagonal_first:
            for table in early:
                early_plane[p].append(share(table.at[core, xy, at_z], plane_peer(p)))

    for k in far_first:
        early_line[k].append(share(guesses.at[core, xy, z], line_peer(k)))
    early_spread(z)

    plane_copies = {}
    for k, load, copy in zip(layers, our_loads, pair_copies):
        load.wait()
        copy.wait_recv()
        for p in diagonal_first:
            at = flipped(xy, p)
            chip = ours[k, at] + pair_recv[k, at].astype(jnp.float32)
            plane_send[k, p - 1] = chip.astype(jnp.bfloat16)
            plane_copies[k, p] = remote(plane_send.at[k, p - 1], plane_recv.at[k, p - 1], plane_peer(p))

    def plane_sum(k):
        total = ours[k, xy] + pair_recv[k, xy].astype(jnp.float32)
        for p in diagonal_first:
            plane_copies[k, p].wait_recv()
            total = total + plane_recv[k, p - 1].astype(jnp.float32)
        return total

    line_copies = []
    for k, near in zip(far_first, reversed(far_first)):
        line_send[k - 1] = plane_sum(k).astype(jnp.bfloat16)
        line_copies.append((k, remote(line_send.at[k - 1], line_recv.at[k - 1], line_peer(k))))

        for copy in early_line[near]:
            copy.wait_recv()
        early_spread(flipped(z, near))
    early_pair = {0: [share(table.at[core, xy], partner) for table in early]}

    grad = plane_sum(0)
    for k, copy in line_copies:
        copy.wait_recv()
        grad = grad + line_recv[k - 1].astype(jnp.float32)
    grad = grad / jnp.float32(count)
    new_m1 = 0.9 * m1[...] + 0.1 * grad
    new_m2 = 0.999 * m2[...] + 0.001 * grad * grad
    update = update_of(new_m1, new_m2, masters[core, xy, z])
    deltas[core, xy, z] = (update - guess.astype(jnp.float32)).astype(jnp.bfloat16)
    update_line = [(k, share(deltas.at[core, xy, z], line_peer(k))) for k in far_first]
    update_plane, update_pair = [], []

    def spread(at_z):
        row = deltas.at[core, xy, at_z]
        for p in diagonal_first:
            update_plane.append((p, at_z, share(row, plane_peer(p))))
        update_pair.append((xy, at_z, share(row, partner)))

    def put_sum(sums, values, side, at, j):
        sums[(side * plane + at) * line + j] = jnp.sum(values * values, axis=0)

    def weight_sums(side, at):
        for j in range(line):
            put_sum(wsums, masters[side, at, j], side, at, j)

    def update_sum(side, at, j):
        values = guesses[side, at, j].astype(jnp.float32) + deltas[side, at, j].astype(jnp.float32)
        put_sum(usums, values, side, at, j)

    spread(z)
    mine[...] = update
    m1_new[...] = new_m1
    m2_new[...] = new_m2
    weight_sums(core, xy)
    for turn, (k, copy) in enumerate(reversed(update_line)):
        copy.wait_recv()
        spread(flipped(z, k))
        if turn == line - 3:
            for p in diagonal_first:
                for early_copy in early_plane[p]:
                    early_copy.wait_recv()
                at = flipped(xy, p)
                early_pair[p] = [share(table.at[core, at], partner) for table in early]
                weight_sums(core, at)
    for j in range(line):
        update_sum(core, xy, j)
    for p, at_z, copy in update_plane:
        copy.wait_recv()
        at = flipped(xy, p)
        update_pair.append((at, at_z, share(deltas.at[core, at, at_z], partner)))
        update_sum(core, at, at_z)

    for p in [0] + diagonal_first:
        for copy in early_pair[p]:
            copy.wait_recv()
        weight_sums(other, flipped(xy, p))
    rows_load.wait()

    index0 = lax.broadcasted_iota(jnp.int32, (count, count), 0)
    index1 = lax.broadcasted_iota(jnp.int32, (count, count), 1)

    def tensor_of(index):
        natural = (index % line * plane + index // line % plane) * 2 + index // (line * plane)
        end = jnp.int32(0)
        tensor = jnp.zeros(index.shape, jnp.int32)
        for k in range(rows_ref.shape[0]):
            end = end + rows_ref[k]
            tensor = tensor + (natural >= end).astype(jnp.int32)
        return tensor

    same = tensor_of(index0) == tensor_of(index1)

    def over_tensor(sums):
        per_row = jnp.sum(jnp.sum(sums[...], axis=1), axis=1, keepdims=True)
        return jnp.sum(jnp.where(same, per_row, 0.0), axis=0, keepdims=True)

    wsq = over_tensor(wsums)

    for at, at_z, copy in update_pair:
        copy.wait_recv()
        update_sum(other, at, at_z)

    ratio = jnp.sqrt(wsq / (over_tensor(usums) + 1e-06))
    column = jnp.sum(jnp.where(index0 == index1, ratio, 0.0), axis=1, keepdims=True)
    ratios[...] = jnp.broadcast_to(0.2 * column, (count, LANES))
    for copy in sent:
        copy.wait_send()


def finish(
    line, plane,
    masters, guesses, deltas, ratios, m1_new, m2_new, mine,
    weights_out, master_out, moment1_out, moment2_out,
    weights, master_new, sem,
):
    me = lax.axis_index("dp")
    copies = [
        pltpu.make_async_copy(m1_new, moment1_out, sem.at[0]),
        pltpu.make_async_copy(m2_new, moment2_out, sem.at[1]),
    ]
    for copy in copies:
        copy.start()

    def scale(side, at, j):
        return ratios[pl.ds((side * plane + at) * line + j, 1), :]

    place = (me % 2, me // 2 % plane, me // (2 * plane))
    master_new[...] = masters[place] - scale(*place) * mine[...]
    copies.append(pltpu.make_async_copy(master_new, master_out, sem.at[2]))
    copies[-1].start()

    @pl.loop(0, line)
    def _(j):
        for at in range(plane):
            for side in range(2):
                update = guesses[side, at, j].astype(jnp.float32) + deltas[side, at, j].astype(jnp.float32)
                new_row = masters[side, at, j] - scale(side, at, j) * update
                weights[j, at, side] = new_row.astype(jnp.bfloat16)
        pltpu.make_async_copy(weights.at[j], weights_out.at[j], sem.at[3 + j]).start()

    for j in range(line):
        copies.append(pltpu.make_async_copy(weights.at[j], weights_out.at[j], sem.at[3 + j]))
    for copy in copies:
        copy.wait()


def pinned(array):
    return pltpu.with_memory_space_constraint(array, pltpu.HBM)


def body(grads, master, moment1, moment2, tensor_rows, step_count):
    count = lax.axis_size("dp")
    line, plane = levels(count)
    row = (master.shape[0] // (8 * LANES), 8, LANES)
    f32, bf16 = jnp.float32, jnp.bfloat16
    hbm = pl.BlockSpec(memory_space=pltpu.HBM)
    vmem = pl.BlockSpec(memory_space=pltpu.VMEM)
    table = (2, plane, line) + row
    gathered = line - 1 + line * (plane - 1)
    remotes = line + gathered + 2 * gathered + 2 * plane + gathered + line * plane
    state = pl.pallas_call(
        functools.partial(kernel, count, line, plane),
        out_shape=(
            jax.ShapeDtypeStruct(table, f32),
            jax.ShapeDtypeStruct(table, bf16),
            jax.ShapeDtypeStruct(table, bf16),
            jax.ShapeDtypeStruct((count, LANES), f32),
            jax.ShapeDtypeStruct(row, f32),
            jax.ShapeDtypeStruct(row, f32),
            jax.ShapeDtypeStruct(row, f32),
        ),
        in_specs=[hbm] * 5 + [pl.BlockSpec(memory_space=pltpu.SMEM)],
        out_specs=(vmem,) * 7,
        scratch_shapes=[
            pltpu.VMEM((line, plane) + row, f32),
            pltpu.VMEM((line, plane) + row, f32),
            pltpu.VMEM((line, plane) + row, bf16),
            pltpu.VMEM((line, plane) + row, bf16),
            pltpu.VMEM((line, plane - 1) + row, bf16),
            pltpu.VMEM((line, plane - 1) + row, bf16),
            pltpu.VMEM((line - 1,) + row, bf16),
            pltpu.VMEM((line - 1,) + row, bf16),
            pltpu.VMEM(row, f32),
            pltpu.VMEM(row, f32),
            pltpu.VMEM((count, 8, LANES), f32),
            pltpu.VMEM((count, 8, LANES), f32),
            pltpu.SMEM(tensor_rows.shape, jnp.int32),
            pltpu.SemaphoreType.DMA((2 * line + 4,)),
            pltpu.SemaphoreType.DMA((remotes,)),
            pltpu.SemaphoreType.DMA((remotes,)),
        ],
        compiler_params=pltpu.CompilerParams(
            collective_id=0, has_side_effects=True, vmem_limit_bytes=40 * 1024 * 1024
        ),
        name="exchange",
    )(
        pinned(grads.reshape((line, plane, 2) + row)),
        pinned(master.reshape(row)), pinned(moment1.reshape(row)), pinned(moment2.reshape(row)),
        pinned(tensor_rows), step_count,
    )
    outs = pl.pallas_call(
        functools.partial(finish, line, plane),
        out_shape=(
            jax.ShapeDtypeStruct((line, plane, 2) + row, bf16),
            jax.ShapeDtypeStruct(row, f32),
            jax.ShapeDtypeStruct(row, f32),
            jax.ShapeDtypeStruct(row, f32),
        ),
        in_specs=[vmem] * 7,
        out_specs=(hbm,) * 4,
        scratch_shapes=[
            pltpu.VMEM((line, plane, 2) + row, bf16),
            pltpu.VMEM(row, f32),
            pltpu.SemaphoreType.DMA((3 + line,)),
        ],
        compiler_params=pltpu.CompilerParams(vmem_limit_bytes=24 * 1024 * 1024),
        name="finish",
    )(*state)
    return tuple(out.reshape(-1) for out in outs)


def solution(mesh):
    placed = (P("dp", None), P("dp"), P("dp"), P("dp"), P(), P())
    return jax.shard_map(
        body,
        mesh=mesh,
        in_specs=placed,
        out_specs=(P(), P("dp"), P("dp"), P("dp")),
        check_vma=False,
    )
```

```python
import functools

import jax
import jax.numpy as jnp
import numpy as np
from jax import lax
from jax.experimental import pallas as pl
from jax.experimental.pallas import tpu as pltpu
from jax.sharding import PartitionSpec as P

LANES = 128
BETA1, BETA2 = 0.9, 0.999
STEP_BITS = 8


def levels(count):
    chips = count // 2
    bits = chips.bit_length() - 1
    plane = 1 << ((bits + 1) // 2)
    return chips // plane, plane


def flipped(value, mask):
    bit = 1
    while bit <= mask:
        if mask & bit:
            value = value + bit * (1 - 2 * (value // bit % 2))
        bit *= 2
    return value


def power(base, step):
    result = jnp.ones(step.shape, jnp.float32)
    for bit in range(STEP_BITS):
        factor = float(np.float32(float(np.float32(base)) ** (2**bit)))
        result = result * jnp.where((step // 2**bit) % 2 == 1, factor, 1.0)
    return result


def kernel(
    count, line, plane,
    grads, master, moment1, moment2, rows_in, step_ref,
    masters, guesses, deltas, ratios, m1_new, m2_new, mine,
    theirs, ours, pair_send, pair_recv, plane_send, plane_recv,
    line_send, line_recv, m1, m2, wsums, usums, rows_ref,
    local_sem, send_sem, recv_sem,
):
    me = lax.axis_index("dp")
    core = me % 2
    xy = me // 2 % plane
    z = me // (2 * plane)
    other = 1 - core
    partner = me + 1 - 2 * core
    far_first = list(range(line - 1, 0, -1))
    diagonal_first = list(range(plane - 1, 0, -1))

    def plane_peer(mask):
        return (z * plane + flipped(xy, mask)) * 2 + core

    def line_peer(mask):
        return (flipped(z, mask) * plane + xy) * 2 + core

    peers = [partner] + [plane_peer(k) for k in range(1, plane)]
    peers += [line_peer(k) for k in range(1, line)]
    barrier = pltpu.get_barrier_semaphore()
    for peer in peers:
        pl.semaphore_signal(barrier, inc=1, device_id=(peer,), device_id_type=pl.DeviceIdType.MESH)

    used = {"local": 0, "remote": 0}
    sent = []

    def local(source, target):
        copy = pltpu.make_async_copy(source, target, local_sem.at[used["local"]])
        used["local"] += 1
        copy.start()
        return copy

    def remote(source, target, peer):
        slot = used["remote"]
        used["remote"] += 1
        copy = pltpu.make_async_remote_copy(
            src_ref=source, dst_ref=target,
            send_sem=send_sem.at[slot], recv_sem=recv_sem.at[slot],
            device_id=(peer,), device_id_type=pl.DeviceIdType.MESH,
        )
        copy.start()
        sent.append(copy)
        return copy

    def share(ref, peer):
        return remote(ref, ref, peer)

    layers = far_first + [0]
    their_loads = [local(grads.at[flipped(z, k), :, other], theirs.at[k]) for k in layers]
    master_load = local(master, masters.at[core, xy, z])
    our_loads = [local(grads.at[flipped(z, k), :, core], ours.at[k]) for k in layers]
    moment_loads = [local(moment1, m1), local(moment2, m2)]
    rows_load = local(rows_in, rows_ref)
    step = jnp.full((8, LANES), step_ref[0], jnp.int32)
    first_scale = 1.0 - power(BETA1, step)
    second_scale = 1.0 - power(BETA2, step)

    def update_of(first, second, weight):
        return (first / first_scale) / (jnp.sqrt(second / second_scale) + 1e-06) + 0.1 * weight


    for k, load in zip(layers, their_loads):
        load.wait()
        pair_send[k] = theirs[k].astype(jnp.bfloat16)
    master_load.wait()
    pl.semaphore_wait(barrier, len(peers))

    pair_copies = [remote(pair_send.at[k], pair_recv.at[k], partner) for k in layers]
    early = (masters, guesses)
    early_line = {k: [share(masters.at[core, xy, z], line_peer(k))] for k in far_first}
    for copy in moment_loads:
        copy.wait()
    guess = update_of(0.9 * m1[...], 0.999 * m2[...], masters[core, xy, z]).astype(jnp.bfloat16)
    guesses[core, xy, z] = guess
    early_plane = {p: [] for p in diagonal_first}

    def early_spread(at_z):
        for p in diagonal_first:
            for table in early:
                early_plane[p].append(share(table.at[core, xy, at_z], plane_peer(p)))

    for k in far_first:
        early_line[k].append(share(guesses.at[core, xy, z], line_peer(k)))

    plane_copies = {}
    for k, load, copy in zip(layers, our_loads, pair_copies):
        load.wait()
        copy.wait_recv()
        for p in diagonal_first:
            at = flipped(xy, p)
            chip = ours[k, at] + pair_recv[k, at].astype(jnp.float32)
            plane_send[k, p - 1] = chip.astype(jnp.bfloat16)
            plane_copies[k, p] = remote(plane_send.at[k, p - 1], plane_recv.at[k, p - 1], plane_peer(p))

    early_spread(z)

    def plane_sum(k):
        total = ours[k, xy] + pair_recv[k, xy].astype(jnp.float32)
        for p in diagonal_first:
            plane_copies[k, p].wait_recv()
            total = total + plane_recv[k, p - 1].astype(jnp.float32)
        return total

    line_copies = []
    for k, near in zip(far_first, reversed(far_first)):
        line_send[k - 1] = plane_sum(k).astype(jnp.bfloat16)
        line_copies.append((k, remote(line_send.at[k - 1], line_recv.at[k - 1], line_peer(k))))

        for copy in early_line[near]:
            copy.wait_recv()
        early_spread(flipped(z, near))
    early_pair = {0: [share(table.at[core, xy], partner) for table in early]}

    grad = plane_sum(0)
    for k, copy in line_copies:
        copy.wait_recv()
        grad = grad + line_recv[k - 1].astype(jnp.float32)
    grad = grad / jnp.float32(count)
    new_m1 = 0.9 * m1[...] + 0.1 * grad
    new_m2 = 0.999 * m2[...] + 0.001 * grad * grad
    update = update_of(new_m1, new_m2, masters[core, xy, z])
    deltas[core, xy, z] = (update - guess.astype(jnp.float32)).astype(jnp.bfloat16)
    update_line = [(k, share(deltas.at[core, xy, z], line_peer(k))) for k in far_first]
    update_plane, update_pair = [], []

    def spread(at_z):
        row = deltas.at[core, xy, at_z]
        for p in diagonal_first:
            update_plane.append((p, at_z, share(row, plane_peer(p))))
        update_pair.append((xy, at_z, share(row, partner)))

    def put_sum(sums, values, side, at, j):
        sums[(side * plane + at) * line + j] = jnp.sum(values * values, axis=0)

    def weight_sums(side, at):
        for j in range(line):
            put_sum(wsums, masters[side, at, j], side, at, j)

    def update_sum(side, at, j):
        values = guesses[side, at, j].astype(jnp.float32) + deltas[side, at, j].astype(jnp.float32)
        put_sum(usums, values, side, at, j)

    spread(z)
    mine[...] = update
    m1_new[...] = new_m1
    m2_new[...] = new_m2
    weight_sums(core, xy)
    for turn, (k, copy) in enumerate(reversed(update_line)):
        copy.wait_recv()
        spread(flipped(z, k))
        if turn == line - 3:
            for p in diagonal_first:
                for early_copy in early_plane[p]:
                    early_copy.wait_recv()
                at = flipped(xy, p)
                early_pair[p] = [share(table.at[core, at], partner) for table in early]
                weight_sums(core, at)
    for j in range(line):
        update_sum(core, xy, j)
    for p, at_z, copy in update_plane:
        copy.wait_recv()
        at = flipped(xy, p)
        update_pair.append((at, at_z, share(deltas.at[core, at, at_z], partner)))
        update_sum(core, at, at_z)

    for p in [0] + diagonal_first:
        for copy in early_pair[p]:
            copy.wait_recv()
        weight_sums(other, flipped(xy, p))
    rows_load.wait()

    index0 = lax.broadcasted_iota(jnp.int32, (count, count), 0)
    index1 = lax.broadcasted_iota(jnp.int32, (count, count), 1)

    def tensor_of(index):
        natural = (index % line * plane + index // line % plane) * 2 + index // (line * plane)
        end = jnp.int32(0)
        tensor = jnp.zeros(index.shape, jnp.int32)
        for k in range(rows_ref.shape[0]):
            end = end + rows_ref[k]
            tensor = tensor + (natural >= end).astype(jnp.int32)
        return tensor

    same = tensor_of(index0) == tensor_of(index1)

    def over_tensor(sums):
        per_row = jnp.sum(jnp.sum(sums[...], axis=1), axis=1, keepdims=True)
        return jnp.sum(jnp.where(same, per_row, 0.0), axis=0, keepdims=True)

    wsq = over_tensor(wsums)

    for at, at_z, copy in update_pair:
        copy.wait_recv()
        update_sum(other, at, at_z)

    ratio = jnp.sqrt(wsq / (over_tensor(usums) + 1e-06))
    column = jnp.sum(jnp.where(index0 == index1, ratio, 0.0), axis=1, keepdims=True)
    ratios[...] = jnp.broadcast_to(0.2 * column, (count, LANES))
    for copy in sent:
        copy.wait_send()


def finish(
    line, plane,
    masters, guesses, deltas, ratios, m1_new, m2_new, mine,
    weights_out, master_out, moment1_out, moment2_out,
    weights, master_new, sem,
):
    me = lax.axis_index("dp")
    copies = [
        pltpu.make_async_copy(m1_new, moment1_out, sem.at[0]),
        pltpu.make_async_copy(m2_new, moment2_out, sem.at[1]),
    ]
    for copy in copies:
        copy.start()

    def scale(side, at, j):
        return ratios[pl.ds((side * plane + at) * line + j, 1), :]

    place = (me % 2, me // 2 % plane, me // (2 * plane))
    master_new[...] = masters[place] - scale(*place) * mine[...]
    copies.append(pltpu.make_async_copy(master_new, master_out, sem.at[2]))
    copies[-1].start()

    @pl.loop(0, line)
    def _(j):
        for at in range(plane):
            for side in range(2):
                update = guesses[side, at, j].astype(jnp.float32) + deltas[side, at, j].astype(jnp.float32)
                new_row = masters[side, at, j] - scale(side, at, j) * update
                weights[j, at, side] = new_row.astype(jnp.bfloat16)
        pltpu.make_async_copy(weights.at[j], weights_out.at[j], sem.at[3 + j]).start()

    for j in range(line):
        copies.append(pltpu.make_async_copy(weights.at[j], weights_out.at[j], sem.at[3 + j]))
    for copy in copies:
        copy.wait()


def pinned(array):
    return pltpu.with_memory_space_constraint(array, pltpu.HBM)


def body(grads, master, moment1, moment2, tensor_rows, step_count):
    count = lax.axis_size("dp")
    line, plane = levels(count)
    row = (master.shape[0] // (8 * LANES), 8, LANES)
    f32, bf16 = jnp.float32, jnp.bfloat16
    hbm = pl.BlockSpec(memory_space=pltpu.HBM)
    vmem = pl.BlockSpec(memory_space=pltpu.VMEM)
    table = (2, plane, line) + row
    gathered = line - 1 + line * (plane - 1)
    remotes = line + gathered + 2 * gathered + 2 * plane + gathered + line * plane
    state = pl.pallas_call(
        functools.partial(kernel, count, line, plane),
        out_shape=(
            jax.ShapeDtypeStruct(table, f32),
            jax.ShapeDtypeStruct(table, bf16),
            jax.ShapeDtypeStruct(table, bf16),
            jax.ShapeDtypeStruct((count, LANES), f32),
            jax.ShapeDtypeStruct(row, f32),
            jax.ShapeDtypeStruct(row, f32),
            jax.ShapeDtypeStruct(row, f32),
        ),
        in_specs=[hbm] * 5 + [pl.BlockSpec(memory_space=pltpu.SMEM)],
        out_specs=(vmem,) * 7,
        scratch_shapes=[
            pltpu.VMEM((line, plane) + row, f32),
            pltpu.VMEM((line, plane) + row, f32),
            pltpu.VMEM((line, plane) + row, bf16),
            pltpu.VMEM((line, plane) + row, bf16),
            pltpu.VMEM((line, plane - 1) + row, bf16),
            pltpu.VMEM((line, plane - 1) + row, bf16),
            pltpu.VMEM((line - 1,) + row, bf16),
            pltpu.VMEM((line - 1,) + row, bf16),
            pltpu.VMEM(row, f32),
            pltpu.VMEM(row, f32),
            pltpu.VMEM((count, 8, LANES), f32),
            pltpu.VMEM((count, 8, LANES), f32),
            pltpu.SMEM(tensor_rows.shape, jnp.int32),
            pltpu.SemaphoreType.DMA((2 * line + 4,)),
            pltpu.SemaphoreType.DMA((remotes,)),
            pltpu.SemaphoreType.DMA((remotes,)),
        ],
        compiler_params=pltpu.CompilerParams(
            collective_id=0, has_side_effects=True, vmem_limit_bytes=40 * 1024 * 1024
        ),
        name="exchange",
    )(
        pinned(grads.reshape((line, plane, 2) + row)),
        pinned(master.reshape(row)), pinned(moment1.reshape(row)), pinned(moment2.reshape(row)),
        pinned(tensor_rows), step_count,
    )
    outs = pl.pallas_call(
        functools.partial(finish, line, plane),
        out_shape=(
            jax.ShapeDtypeStruct((line, plane, 2) + row, bf16),
            jax.ShapeDtypeStruct(row, f32),
            jax.ShapeDtypeStruct(row, f32),
            jax.ShapeDtypeStruct(row, f32),
        ),
        in_specs=[vmem] * 7,
        out_specs=(hbm,) * 4,
        scratch_shapes=[
            pltpu.VMEM((line, plane, 2) + row, bf16),
            pltpu.VMEM(row, f32),
            pltpu.SemaphoreType.DMA((3 + line,)),
        ],
        compiler_params=pltpu.CompilerParams(vmem_limit_bytes=24 * 1024 * 1024),
        name="finish",
    )(*state)
    return tuple(out.reshape(-1) for out in outs)


def solution(mesh):
    placed = (P("dp", None), P("dp"), P("dp"), P("dp"), P(), P())
    return jax.shard_map(
        body,
        mesh=mesh,
        in_specs=placed,
        out_specs=(P(), P("dp"), P("dp"), P("dp")),
        check_vma=False,
    )
```
